32 devices in a mesh: dp: 16 (over z, x, core), mp: 2 (over y).
Axes of the slice: x: 2, y: 2, z: 4, core: 2. Of those that a mesh axis runs over, the one named last changes fastest.
Arguments:
- tokens: bfloat16 [8192, 8192], P('dp'), may hold values from -6 to 6
- queries: bfloat16 [8192, 64, 128], P('dp', 'mp'), may hold values from -68 to 68
- out_grad: bfloat16 [8192, 64, 128], P('dp', 'mp'), may hold values from -6 to 6
- segment_ids: int32 [16, 512], P('dp'), may hold values from 0 to 3, never falling along the last dimension, each value on 1 to 256 neighbouring positions
- weight_slots: bfloat16 [16384, 8, 2, 128], P('dp', 'mp'), may hold values from -0.0625 to 0.0625
- old_place: int32 [64], replicated, may hold values from 0 to 127, as said below
- new_place: int32 [64], replicated, may hold values from 0 to 127, as said below
Outputs:
- input_grad: bfloat16 [8192, 8192], P('dp', 'mp')
- query_grad: bfloat16 [8192, 64, 128], P('dp', 'mp')
- weight_grad: float32 [16384, 8, 2, 128], P('dp', 'mp')
The draws below stay inside these ranges and needn't reach their ends.
Inputs may be any that keep to these rules, and one draw needn't show every extreme that they name: `old_place`: entries are distinct slot numbers; slot s lies on index s // 8 of dp; some index of dp holds 8 blocks. `new_place`: entries are distinct slot numbers; slot s lies on index s // 8 of dp; some index of dp receives 8 blocks.
All inputs are finite; a program needn't handle non-finite values.
Results may differ from the reference program's by a relative error of at most 0.018.
Values may be sent and summed in bfloat16 or wider, within the bound.
A program may use at most 192 MiB of HBM per device.

```python
import math
import jax
import jax.numpy as jnp
import numpy as np
from jax import lax

D = 8192
QH = 64
KVH = 8
HD = 128
BR = 128
TOK = 512
BLOCKS = 64
SLOTS = 8
TOKENS = 8192
N_DP = 16


def place_blocks(key):
    slot_count = N_DP * SLOTS
    first_key, second_key = jax.random.split(key)
    shuffled = jax.random.permutation(first_key, slot_count).astype(jnp.int32)
    busiest = jax.random.randint(second_key, (), 0, N_DP).astype(jnp.int32)
    owner_dev = jnp.arange(slot_count, dtype=jnp.int32) // SLOTS
    priority = shuffled - (owner_dev == busiest).astype(jnp.int32) * slot_count
    ordered = jnp.argsort(priority, stable=True).astype(jnp.int32)
    return ordered[:BLOCKS]


def draw_old_place(key, part):
    return place_blocks(jax.random.fold_in(key, 11))


def draw_new_place(key, part):
    return place_blocks(jax.random.fold_in(key, 23))


def draw_queries(key, part):
    base_key = jax.random.fold_in(key, 0)
    base = jnp.clip(jax.random.normal(base_key, (TOKENS, QH, HD), jnp.float32), -6.0, 6.0)
    return base.astype(jnp.bfloat16)


def strengthened(drawn, own_key, source, target, blocks, factor):
    owner, partner = [(jnp.arange(drawn.shape[axis_at]) // (drawn.shape[axis_at] // blocks)).reshape([-1 if axis == axis_at else 1 for axis in range(drawn.ndim)]) for axis_at in (source, target)]
    chosen = jax.random.permutation(own_key, blocks)[partner]
    strong = (owner == chosen) | (owner == (partner + blocks // 2) % blocks)
    return jnp.where(strong, factor * drawn, drawn)


def block_scale(own_key, extent, cuts, smallest, top_value):
    level = 1.0
    for dim, parts in cuts:
        heights = jax.random.uniform(jax.random.fold_in(jax.random.fold_in(own_key, 6), dim), (parts,), jnp.float32, smallest / len(cuts), top_value / len(cuts))
        level = level * jnp.repeat(jnp.exp(heights), extent[dim] // parts).reshape((-1,) + (1,) * (len(extent) - 1 - dim))
    return level


def length_profile(number_of, total, reach, skew):
    portions = [(1 << 20) // math.isqrt(standing ** skew) + 1 for standing in range(2, number_of + 1)]
    rest, given = total - reach - (number_of - 1), [1] * (number_of - 1)
    while rest > 0:
        candidates = [i for i in range(number_of - 1) if given[i] < reach]
        whole, budget = sum([portions[i] for i in candidates]), rest
        for i in candidates:
            more = min(reach - given[i], max(1, budget * portions[i] // whole), rest)
            given[i] = given[i] + more
            rest = rest - more
    return np.array([reach] + given)


def uneven_parts(key, count, total, bound, slope):
    if count == 2:
        one = jax.random.randint(key, (), max(1, total - bound), min(bound, total - 1) + 1)
        return jnp.stack([one, total - one])
    sizes = jnp.asarray(length_profile(count, total, bound, slope), jnp.int32)
    pairs = (count - 1) // 2
    source_of, taker = sizes[1:1 + 2 * pairs:2], sizes[2:2 + 2 * pairs:2]
    margin = jnp.minimum(source_of - 1, bound - taker)
    moved = jax.random.randint(jax.random.fold_in(key, 1), (pairs,), 0, 1 << 20) % (margin + 1)
    sizes = sizes.at[1:1 + 2 * pairs:2].set(source_of - moved).at[2:2 + 2 * pairs:2].set(taker + moved)
    return sizes[jax.random.permutation(jax.random.fold_in(key, 2), count)]


def centred(rng, shape, spread, reach, cuts=(), kind=jnp.bfloat16):
    gain = block_scale(rng, shape, cuts, -0.22, 0.18) if cuts else 1.0
    array = jax.random.normal(rng, shape, jnp.float32) * spread * gain
    return jnp.minimum(jnp.maximum(array, -reach), reach).astype(kind)


def heavy_noise(rng, shape, width, reach, cuts, heavy, kind=jnp.bfloat16):
    entries = width * jax.random.normal(rng, shape, jnp.float32)
    if cuts:
        entries = entries * block_scale(rng, shape, cuts, -0.22, 0.18)
    return jnp.clip(strengthened(entries, jax.random.fold_in(rng, 3), *heavy), -reach, reach).astype(kind)


def setup_inputs(seed: int = 0) -> dict:
    streams_of = jax.random.split(jax.random.key(seed), 8)
    tokens = heavy_noise(streams_of[0], (TOKENS, D), 1.0, 6.0, ((0, 16),), (0, 1, 16, 2.0))
    queries = draw_queries(jax.random.fold_in(streams_of[7], 71), 0)
    out_grad = centred(streams_of[2], (TOKENS, QH, HD), 1.0, 6.0, ((0, 16), (1, 2)))
    segment_ids = jax.vmap(lambda own: jnp.searchsorted(jnp.cumsum(uneven_parts(own, 4, TOK, TOK // 2, 0)), jnp.arange(TOK), side="right"))(jax.random.split(streams_of[3], N_DP)).reshape((N_DP, TOK)).astype(jnp.int32)
    weight_slots = centred(streams_of[4], (N_DP * SLOTS * BR, KVH, 2, HD), D ** -0.5, 0.0625, ((0, 16), (1, 2)))
    old_place = draw_old_place(jax.random.fold_in(streams_of[7], 71), 0)
    new_place = draw_new_place(jax.random.fold_in(streams_of[7], 71), 0)
    return dict(tokens=tokens, queries=queries, out_grad=out_grad, segment_ids=segment_ids, weight_slots=weight_slots, old_place=old_place, new_place=new_place)


def attend(tokens, weights, queries, out_grad, seg_row):
    tok_count = tokens.shape[0]
    model_width = weights.shape[0]
    head_count = weights.shape[1]
    head_size = weights.shape[3]
    per_head = queries.shape[1] // head_count
    half_size = head_size // 2
    projected = jnp.dot(tokens, weights.reshape(model_width, head_count * 2 * head_size), preferred_element_type=jnp.float32)
    projected = projected.reshape(tok_count, head_count, 2, head_size)
    frequency = 500000.0 ** (-2.0 * jnp.arange(half_size, dtype=jnp.float32) / head_size)
    angle_tab = jnp.arange(tok_count, dtype=jnp.float32)[:, None] * frequency[None, :]
    cos_tab = jnp.cos(angle_tab)[:, None, :]
    sin_tab = jnp.sin(angle_tab)[:, None, :]
    lower_half = projected[:, :, 0, :half_size]
    upper_half = projected[:, :, 0, half_size:]
    rot_keys = jnp.concatenate([lower_half * cos_tab - upper_half * sin_tab, upper_half * cos_tab + lower_half * sin_tab], axis=-1).astype(jnp.bfloat16)
    values = projected[:, :, 1].astype(jnp.bfloat16)
    inv_root = 1.0 / jnp.sqrt(jnp.float32(head_size))
    query_wide = queries.reshape(tok_count, head_count, per_head, head_size).astype(jnp.float32)
    outgrad_wide = out_grad.reshape(tok_count, head_count, per_head, head_size).astype(jnp.float32)
    key_wide = rot_keys.astype(jnp.float32)
    value_wide = values.astype(jnp.float32)
    scores = jnp.einsum('qhgd,khd->hgqk', query_wide, key_wide) * inv_root
    position = jnp.arange(tok_count)
    allowed = (position[:, None] >= position[None, :]) & (seg_row[:, None] == seg_row[None, :])
    scores = jnp.where(allowed, scores, jnp.float32(-1e+30))
    row_max = lax.optimization_barrier(jnp.max(scores, axis=-1, keepdims=True))
    exp_scores = jnp.exp(scores - row_max)
    attn_prob = exp_scores / lax.optimization_barrier(jnp.sum(exp_scores, axis=-1, keepdims=True))
    prob_half = lax.optimization_barrier(attn_prob.astype(jnp.bfloat16)).astype(jnp.float32)
    attn_out = jnp.einsum('hgqk,khd->qhgd', prob_half, value_wide)
    row_dot = lax.optimization_barrier(jnp.sum(outgrad_wide * attn_out, axis=-1))
    prob_grad = jnp.einsum('qhgd,khd->hgqk', outgrad_wide, value_wide)
    score_grad = attn_prob * (prob_grad - jnp.transpose(row_dot, (1, 2, 0))[..., None])
    score_half = lax.optimization_barrier(score_grad.astype(jnp.bfloat16)).astype(jnp.float32)
    query_grad = (jnp.einsum('hgqk,khd->qhgd', score_half, key_wide) * inv_root).reshape(tok_count, head_count * per_head, head_size).astype(jnp.bfloat16)
    rot_grad = jnp.einsum('hgqk,qhgd->khd', score_half, query_wide) * inv_root
    value_grad = jnp.einsum('hgqk,qhgd->khd', prob_half, outgrad_wide)
    grad_lower = rot_grad[..., :half_size]
    grad_upper = rot_grad[..., half_size:]
    key_grad = jnp.concatenate([grad_lower * cos_tab + grad_upper * sin_tab, grad_upper * cos_tab - grad_lower * sin_tab], axis=-1)
    pair_grad = jnp.stack([key_grad, value_grad], axis=2).astype(jnp.bfloat16)
    return (query_grad, pair_grad)

def reference(tokens, queries, out_grad, segment_ids, weight_slots, old_place, new_place):
    in_block = jnp.arange(BR, dtype=jnp.int32)
    old_index = (old_place.astype(jnp.int32)[:, None] * BR + in_block[None, :]).reshape(-1)
    weights = jnp.take(weight_slots, old_index, axis=0)
    weight_flat = weights.reshape(D, KVH * 2 * HD)

    def per_sequence(grad_acc, inputs):
        seq_tokens, seq_queries, seq_outgrad, seq_ids = inputs
        query_grad, pair_grad = attend(seq_tokens, weights, seq_queries, seq_outgrad, seq_ids)
        pair_flat = pair_grad.reshape(TOK, KVH * 2 * HD)
        seq_part = lax.dot_general(seq_tokens, pair_flat, (((0,), (0,)), ((), ())), preferred_element_type=jnp.float32).astype(jnp.bfloat16)
        grad_acc = grad_acc + lax.optimization_barrier(seq_part).astype(jnp.float32)
        input_grad = lax.dot_general(pair_flat, weight_flat, (((1,), (1,)), ((), ())), preferred_element_type=jnp.float32).astype(jnp.bfloat16)
        return (grad_acc, (input_grad, query_grad))
    stacked = (tokens.reshape(N_DP, TOK, D), queries.reshape(N_DP, TOK, QH, HD), out_grad.reshape(N_DP, TOK, QH, HD), segment_ids)
    grad_sum, (input_grads, query_grads) = lax.scan(per_sequence, jnp.zeros((D, KVH * 2 * HD), jnp.float32), stacked)
    slot_ids = jnp.arange(N_DP * SLOTS, dtype=jnp.int32)
    matched = (new_place.astype(jnp.int32)[None, :] == slot_ids[:, None]).astype(jnp.int32)
    slot_block = lax.optimization_barrier(jnp.sum(matched * jnp.arange(BLOCKS, dtype=jnp.int32)[None, :], axis=1))
    slot_used = lax.optimization_barrier(jnp.sum(matched, axis=1)).astype(jnp.float32)
    row_index = (slot_block[:, None] * BR + in_block[None, :]).reshape(-1)
    row_keep = jnp.repeat(slot_used, BR)
    weight_grad = jnp.take(grad_sum, row_index, axis=0) * row_keep[:, None]
    return (input_grads.reshape(TOKENS, D), query_grads.reshape(TOKENS, QH, HD), weight_grad.reshape(N_DP * SLOTS * BR, KVH, 2, HD))
```

```python
import functools

import jax
import jax.numpy as jnp
from jax import lax
from jax.experimental import pallas as pl
from jax.experimental.pallas import tpu as pltpu
from jax.sharding import PartitionSpec as P

BR = 128
LOG2E = 1.4426950408889634
VMEM_LIMIT = 60 * 1024 * 1024


def params():
    return pltpu.CompilerParams(
        dimension_semantics=("arbitrary",), vmem_limit_bytes=VMEM_LIMIT
    )


def group_of(count):
    for size in (8, 4, 2):
        if count % size == 0:
            return size
    return 1


def block_specs(group, width):
    return [
        pl.BlockSpec((BR, width), functools.partial(lambda r, i, p: (p[i * group + r], 0), r))
        for r in range(group)
    ]


def project_kernel(group, head_size, place, tok_ref, cos_ref, sin_ref, *refs):
    blocks, out_ref, total = refs[:group], refs[group], refs[group + 1]
    step = pl.program_id(0)

    @pl.when(step == 0)
    def _():
        total[...] = jnp.zeros_like(total)

    w = jnp.concatenate([b[...] for b in blocks], axis=0)
    total[...] += jnp.dot(tok_ref[...], w, preferred_element_type=jnp.float32)

    @pl.when(step == pl.num_programs(0) - 1)
    def _():
        pair = 2 * head_size
        for h in range(total.shape[1] // pair):
            key = total[:, h * pair : h * pair + head_size]
            rot = key * cos_ref[...] + pltpu.roll(key, head_size // 2, 1) * sin_ref[...]
            out_ref[:, h * pair : h * pair + head_size] = rot.astype(jnp.bfloat16)
            value = total[:, h * pair + head_size : (h + 1) * pair]
            out_ref[:, h * pair + head_size : (h + 1) * pair] = value.astype(jnp.bfloat16)


def project(tokens, gathered, place, cos_tab, sin_tab, head_size):
    tok_count = tokens.shape[0]
    width = gathered.shape[1]
    count = place.shape[0]
    group = group_of(count)
    table = pl.BlockSpec((tok_count, head_size), lambda i, p: (0, 0))
    return pl.pallas_call(
        functools.partial(project_kernel, group, head_size),
        out_shape=jax.ShapeDtypeStruct((tok_count, width), jnp.bfloat16),
        grid_spec=pltpu.PrefetchScalarGridSpec(
            num_scalar_prefetch=1,
            grid=(count // group,),
            in_specs=[pl.BlockSpec((tok_count, group * BR), lambda i, p: (0, i)), table, table]
            + block_specs(group, width),
            out_specs=pl.BlockSpec((tok_count, width), lambda i, p: (0, 0)),
            scratch_shapes=[pltpu.VMEM((tok_count, width), jnp.float32)],
        ),
        compiler_params=params(),
        cost_estimate=pl.CostEstimate(
            flops=2 * tok_count * count * BR * width,
            bytes_accessed=2 * (tok_count * count * BR + count * BR * width + tok_count * width),
            transcendentals=0,
        ),
        name="project",
    )(place, tokens, cos_tab, sin_tab, *([gathered] * group))


def attend_kernel(
    per_head, tile, q_ref, og_ref, kv_ref, col_ref, row_ref, cos_ref, sin_ref,
    dq_ref, pair_ref, bias, key_t, rot_acc, val_acc,
):
    tok_count, pair = kv_ref.shape
    hd = pair // 2
    inv_root = 1.0 / (hd ** 0.5)

    @pl.when(pl.program_id(0) == 0)
    def _():
        kpos = lax.broadcasted_iota(jnp.int32, bias.shape, 0)
        qpos = lax.broadcasted_iota(jnp.int32, bias.shape, 1)
        allowed = (kpos <= qpos) & (col_ref[...] == row_ref[...])
        bias[...] = jnp.where(allowed, 0.0, -1e30).astype(jnp.float32)

    key_t[...] = kv_ref[:, :hd].astype(jnp.float32).T.astype(jnp.bfloat16)
    rot_acc[...] = jnp.zeros_like(rot_acc)
    val_acc[...] = jnp.zeros_like(val_acc)

    def head(j, carry):
        lanes = pl.ds(pl.multiple_of(j * hd, hd), hd)
        for t in range(tok_count // tile):
            rows = slice(t * tile, (t + 1) * tile)
            reach = (t + 1) * tile
            q = q_ref[rows, lanes]
            og = og_ref[rows, lanes]
            nt = (((1,), (1,)), ((), ()))
            s = lax.dot_general(kv_ref[:reach, :hd], q, nt, preferred_element_type=jnp.float32)
            s = s * (inv_root * LOG2E) + bias[:reach, rows]
            e = jnp.exp2(s - jnp.max(s, axis=0, keepdims=True))
            p = e * (1.0 / jnp.sum(e, axis=0, keepdims=True))
            pb = p.astype(jnp.bfloat16)
            dp = lax.dot_general(kv_ref[:reach, hd:], og, nt, preferred_element_type=jnp.float32)
            dot = jnp.sum(pb.astype(jnp.float32) * dp, axis=0, keepdims=True)
            ds = (p * (dp - dot)).astype(jnp.bfloat16)
            val_acc[:reach, :] += jnp.dot(pb, og, preferred_element_type=jnp.float32)
            rot_acc[:reach, :] += jnp.dot(ds, q, preferred_element_type=jnp.float32)
            dq = jnp.dot(key_t[:, :reach], ds, preferred_element_type=jnp.float32)
            dq_ref[rows, lanes] = (dq * inv_root).T.astype(jnp.bfloat16)
        return carry

    lax.fori_loop(0, per_head, head, 0, unroll=2)
    g = rot_acc[...] * inv_root
    back = g * cos_ref[...] - pltpu.roll(g, hd // 2, 1) * sin_ref[...]
    pair_ref[:, :hd] = back.astype(jnp.bfloat16)
    pair_ref[:, hd:] = val_acc[...].astype(jnp.bfloat16)


def attend(queries, out_grad, pairs, seg_row, cos_tab, sin_tab, head_count, head_size):
    tok_count, q_width = queries.shape
    per_head = q_width // head_count // head_size
    tile = tok_count // 2 if tok_count % 512 == 0 else tok_count
    slab = pl.BlockSpec((tok_count, per_head * head_size), lambda h: (0, h))
    both = pl.BlockSpec((tok_count, 2 * head_size), lambda h: (0, h))
    table = pl.BlockSpec((tok_count, head_size), lambda h: (0, 0))
    col = pl.BlockSpec((tok_count, 1), lambda h: (0, 0))
    row = pl.BlockSpec((1, tok_count), lambda h: (0, 0))
    return pl.pallas_call(
        functools.partial(attend_kernel, per_head, tile),
        out_shape=(
            jax.ShapeDtypeStruct(queries.shape, jnp.bfloat16),
            jax.ShapeDtypeStruct(pairs.shape, jnp.bfloat16),
        ),
        grid=(head_count,),
        in_specs=[slab, slab, both, col, row, table, table],
        out_specs=(slab, both),
        scratch_shapes=[
            pltpu.VMEM((tok_count, tok_count), jnp.float32),
            pltpu.VMEM((head_size, tok_count), jnp.bfloat16),
            pltpu.VMEM((tok_count, head_size), jnp.float32),
            pltpu.VMEM((tok_count, head_size), jnp.float32),
        ],
        compiler_params=params(),
        cost_estimate=pl.CostEstimate(
            flops=10 * tok_count * tok_count * q_width,
            bytes_accessed=6 * tok_count * q_width + 4 * tok_count * pairs.shape[1],
            transcendentals=tok_count * tok_count * q_width // head_size,
        ),
        name="attend",
    )(queries, out_grad, pairs, seg_row.reshape(-1, 1), seg_row, cos_tab, sin_tab)


def parts_kernel(group, block_of, used, tok_ref, pair_ref, out_ref):
    step = pl.program_id(0)
    for r in range(group):
        slot = step * group + r
        rows = slice(r * BR, (r + 1) * BR)

        @pl.when(used[slot] != 0)
        def _():
            cols = pl.ds(pl.multiple_of(block_of[slot] * BR, BR), BR)
            out_ref[rows, :] = lax.dot_general(
                tok_ref[:, cols], pair_ref[...], (((0,), (0,)), ((), ())),
                preferred_element_type=jnp.float32,
            ).astype(jnp.bfloat16)

        @pl.when(used[slot] == 0)
        def _():
            out_ref[rows, :] = jnp.zeros((BR, out_ref.shape[1]), jnp.bfloat16)


def slot_parts(tokens, pairs, block_of, used):
    slot_total = block_of.shape[0]
    group = group_of(slot_total)
    width = pairs.shape[1]
    return pl.pallas_call(
        functools.partial(parts_kernel, group),
        out_shape=jax.ShapeDtypeStruct((slot_total * BR, width), jnp.bfloat16),
        grid_spec=pltpu.PrefetchScalarGridSpec(
            num_scalar_prefetch=2,
            grid=(slot_total // group,),
            in_specs=[
                pl.BlockSpec(tokens.shape, lambda i, b, u: (0, 0)),
                pl.BlockSpec(pairs.shape, lambda i, b, u: (0, 0)),
            ],
            out_specs=pl.BlockSpec((group * BR, width), lambda i, b, u: (i, 0)),
        ),
        compiler_params=params(),
        cost_estimate=pl.CostEstimate(
            flops=2 * tokens.size * width,
            bytes_accessed=2 * (tokens.size + slot_total * BR * width),
            transcendentals=0,
        ),
        name="slot_parts",
    )(block_of, used, tokens, pairs)


def input_kernel(group, add, place, pair_ref, *refs):
    blocks, out_ref = refs[:group], refs[-1]
    w = jnp.concatenate([b[...] for b in blocks], axis=0)
    total = lax.dot_general(
        pair_ref[...], w, (((1,), (1,)), ((), ())), preferred_element_type=jnp.float32
    )
    if add:
        total = total + refs[group][...].astype(jnp.float32)
    out_ref[...] = total.astype(jnp.bfloat16)


def input_part(pairs, gathered, place, other=None):
    tok_count, width = pairs.shape
    count = place.shape[0]
    group = group_of(count)
    wide = pl.BlockSpec((tok_count, group * BR), lambda i, p: (0, i))
    add = other is not None
    return pl.pallas_call(
        functools.partial(input_kernel, group, add),
        out_shape=jax.ShapeDtypeStruct((tok_count, count * BR), jnp.bfloat16),
        grid_spec=pltpu.PrefetchScalarGridSpec(
            num_scalar_prefetch=1,
            grid=(count // group,),
            in_specs=[pl.BlockSpec(pairs.shape, lambda i, p: (0, 0))]
            + block_specs(group, width)
            + ([wide] if add else []),
            out_specs=wide,
        ),
        compiler_params=params(),
        cost_estimate=pl.CostEstimate(
            flops=2 * tok_count * width * count * BR,
            bytes_accessed=2 * (count * BR * width + 2 * tok_count * count * BR),
            transcendentals=0,
        ),
        name="input_own" if add else "input_other",
    )(place, pairs, *([gathered] * group), *((other,) if add else ()))


def local(tokens, queries, out_grad, segment_ids, weight_slots, old_place, new_place):
    tok_count = tokens.shape[0]
    slot_rows, head_count, _, head_size = weight_slots.shape
    width = head_count * 2 * head_size
    dp_count = lax.axis_size("dp")
    mp_count = lax.axis_size("mp")
    slot_total = dp_count * (slot_rows // BR)
    block_count = old_place.shape[0]

    gathered = lax.all_gather(weight_slots.reshape(slot_rows, width), "dp", axis=0, tiled=True)

    half = head_size // 2
    frequency = 500000.0 ** (-2.0 * jnp.arange(half, dtype=jnp.float32) / head_size)
    angle = jnp.arange(tok_count, dtype=jnp.float32)[:, None] * frequency[None, :]
    cos_half, sin_half = jnp.cos(angle), jnp.sin(angle)
    cos_tab = jnp.concatenate([cos_half, cos_half], axis=1)
    sin_tab = jnp.concatenate([-sin_half, sin_half], axis=1)

    pairs = project(tokens, gathered, old_place, cos_tab, sin_tab, head_size)
    query_grad, pair_grad = attend(
        queries.reshape(tok_count, -1), out_grad.reshape(tok_count, -1), pairs, segment_ids,
        cos_tab, sin_tab, head_count, head_size,
    )

    slot_ids = jnp.arange(slot_total, dtype=jnp.int32)
    matched = (new_place[None, :] == slot_ids[:, None]).astype(jnp.int32)
    block_of = jnp.sum(matched * jnp.arange(block_count, dtype=jnp.int32)[None, :], axis=1)
    used = jnp.sum(matched, axis=1)
    term = slot_parts(tokens, pair_grad, block_of, used)
    term, pair_later, query_grad = lax.optimization_barrier((term, pair_grad, query_grad))
    weight_grad = lax.psum_scatter(term, "dp", scatter_dimension=0, tiled=True)

    me = lax.axis_index("mp")
    share = old_place.reshape(mp_count, block_count // mp_count)
    total = None
    for gap in range(1, mp_count):
        target = lax.rem(me + gap, mp_count)
        places = lax.dynamic_index_in_dim(share, target, 0, keepdims=False)
        piece = input_part(pair_later, gathered, places)
        ring = [(i, (i + gap) % mp_count) for i in range(mp_count)]
        arrived = lax.ppermute(piece, "mp", ring)
        total = arrived if total is None else total + arrived
    mine = lax.dynamic_index_in_dim(share, me, 0, keepdims=False)
    input_grad = input_part(pair_later, gathered, mine, total)
    return (
        input_grad,
        query_grad.reshape(queries.shape),
        weight_grad.astype(jnp.float32).reshape(slot_rows, head_count, 2, head_size),
    )


def solution(mesh):
    return jax.shard_map(
        local,
        mesh=mesh,
        in_specs=(
            P("dp", None),
            P("dp", "mp", None),
            P("dp", "mp", None),
            P("dp", None),
            P("dp", "mp", None, None),
            P(),
            P(),
        ),
        out_specs=(P("dp", "mp"), P("dp", "mp", None), P("dp", "mp", None, None)),
        check_vma=False,
    )
```
